32 devices in a mesh: atoms: 16 (over z, y, x), vecs: 2 (over core).
Axes of the slice: x: 2, y: 2, z: 4, core: 2. Of those that a mesh axis runs over, the one named last changes fastest.
Arguments:
- start_block: bfloat16 [8192, 1024], P('atoms', 'vecs'), may hold values from -6 to 6
- onsite: bfloat16 [64, 128, 128], P('atoms'), may hold values from -0.15625 to 0.15625
- hopping: bfloat16 [64, 4, 128, 128], P('atoms'), as said below
- columns: int32 [64, 4], P('atoms'), may hold values from 0 to 63, as said below
- counts: int32 [64], P('atoms'), may hold values from 0 to 4, as said below
Outputs:
- filtered: bfloat16 [8192, 1024], P('atoms', 'vecs')
- gram: float32 [1024, 1024], P('atoms', 'vecs')
- projected: float32 [1024, 1024], P('atoms', 'vecs')
The draws below stay inside these ranges and needn't reach their ends.
Inputs may be any that keep to these rules, and one draw needn't show every extreme that they name: `columns`: each block row lists its live neighbours in its first counts[i] slots; every neighbour lies at most 2 blocks away, counted cyclically over the 64 blocks; the neighbour relation is symmetric; the other slots name blocks within the same reach that are not neighbours. `counts`: some block row has all 4 slots live. For a live slot, hopping[j, t] with columns[j, t] = i is the transpose of hopping[i, s] with columns[i, s] = j.
All inputs are finite; a program needn't handle non-finite values.
Results may differ from the reference program's by a relative error of at most 0.0098.
Values may be sent and summed in bfloat16 or wider, within the bound.
A program may use at most 64 MiB of HBM per device.

```python
import jax
import jax.numpy as jnp
from jax import lax

BLK = 128
REACH = 2
M = 1024
DEG = 12
SLOTS = 4
NBLK = 64
NROWS = 8192


def neighbour_graph(key):
    base_key = jax.random.fold_in(key, 9071)
    density = jax.random.randint(jax.random.fold_in(base_key, 1), (NBLK,), 30, 100)
    edge_rolls = jax.random.randint(jax.random.fold_in(base_key, 2), (NBLK, REACH), 0, 100)
    forward = (edge_rolls < density[:, None]).astype(jnp.int32)
    forward = forward.at[0, :].set(1)
    for reach_step in range(REACH):
        forward = forward.at[NBLK - reach_step - 1, reach_step].set(1)
    backward = jnp.stack([jnp.roll(forward[:, reach_step], reach_step + 1) for reach_step in range(REACH)], axis=1)
    blocks = jnp.arange(NBLK, dtype=jnp.int32)
    offsets = jnp.arange(1, REACH + 1, dtype=jnp.int32)
    targets = jnp.concatenate([jnp.mod(blocks[:, None] + offsets[None, :], NBLK), jnp.mod(blocks[:, None] - offsets[None, :], NBLK)], axis=1)
    live_slot = jnp.concatenate([forward, backward], axis=1)
    order_key = (1 - live_slot) * SLOTS + jnp.arange(SLOTS, dtype=jnp.int32)[None, :]
    slot_order = jnp.argsort(order_key, axis=1, stable=True)
    columns = jnp.take_along_axis(targets, slot_order, axis=1).astype(jnp.int32)
    counts = jnp.sum(live_slot, axis=1).astype(jnp.int32)
    return (columns, counts)


def draw_columns(key, part):
    return neighbour_graph(key)[0]


def draw_counts(key, part):
    return neighbour_graph(key)[1]


def draw_hopping(key, part):
    columns, counts = neighbour_graph(key)
    row_ids = jnp.broadcast_to(jnp.arange(NBLK, dtype=jnp.int32)[:, None], columns.shape)
    low_id = jnp.minimum(row_ids, columns)
    high_id = jnp.maximum(row_ids, columns)
    pair_ids = (low_id * NBLK + high_id).reshape(-1)
    block_key = jax.random.fold_in(key, 5113)

    def one_block(pair_id):
        return jax.random.normal(jax.random.fold_in(block_key, pair_id), (BLK, BLK), jnp.float32)
    drawn = jax.vmap(one_block)(pair_ids).reshape(NBLK, SLOTS, BLK, BLK)
    transposed = (row_ids > columns)[:, :, None, None]
    drawn = jnp.where(transposed, jnp.swapaxes(drawn, 2, 3), drawn)
    hop_scale = 1.0 / jnp.sqrt(jnp.float32(BLK * (SLOTS + 1)))
    return (drawn * hop_scale).astype(jnp.bfloat16)


def level_of(rng, dims, split, smallest, top_value):
    factor_of = 1.0
    for dim, parts in split:
        heights = jax.random.uniform(jax.random.fold_in(jax.random.fold_in(rng, 6), dim), (parts,), jnp.float32, smallest / len(split), top_value / len(split))
        factor_of = factor_of * jnp.repeat(jnp.exp(heights), dims[dim] // parts).reshape((-1,) + (1,) * (len(dims) - 1 - dim))
    return factor_of


def gaussian(stream_key, extent, scale, reach, shards=(), kind=jnp.bfloat16):
    values = jax.random.normal(stream_key, extent, jnp.float32) * scale
    if len(shards) > 0:
        values = level_of(stream_key, extent, shards, -0.22, 0.18) * values
    return jnp.clip(values, min=-reach, max=reach).astype(kind)


def setup_inputs(seed: int = 0) -> dict:
    keys = jax.random.split(jax.random.key(seed), 6)
    return {
        "start_block": gaussian(keys[0], (NROWS, M), 1.0, 6.0, ((0, 16), (1, 2))),
        "onsite": gaussian(keys[1], (NBLK, BLK, BLK), (2 * BLK * (SLOTS + 1)) ** -0.5, 0.15625, ((0, 16),)),
        "hopping": draw_hopping(jax.random.fold_in(keys[5], 71), 0),
        "columns": draw_columns(jax.random.fold_in(keys[5], 71), 0),
        "counts": draw_counts(jax.random.fold_in(keys[5], 71), 0),
    }


filter_low = -0.5
filter_top = 4.0
filter_bottom = -1.6


def filter_coefficients(degree):
    center = 0.5 * (filter_top + filter_low)
    half_width = 0.5 * (filter_top - filter_low)
    sigma_first = half_width / (filter_bottom - center)
    listed = [(sigma_first / half_width, 0.0)]
    sigma_now = sigma_first
    for degree_step in range(1, degree):
        sigma_next = 1.0 / (2.0 / sigma_first - sigma_now)
        listed.append((2.0 * sigma_next / half_width, sigma_now * sigma_next))
        sigma_now = sigma_next
    return center, listed


def apply_operator(vectors, onsite, hopping, columns, counts):
    as_wide = vectors.astype(jnp.float32)
    onsite_wide = onsite.astype(jnp.float32)
    summed = 0.5 * (jnp.einsum("rij,rjc->ric", onsite_wide, as_wide) + jnp.einsum("rji,rjc->ric", onsite_wide, as_wide))
    live_slot = jnp.arange(SLOTS, dtype=jnp.int32)[None, :] < counts[:, None]
    for slot_index in range(SLOTS):
        weights = jnp.where(live_slot[:, slot_index, None, None], hopping[:, slot_index].astype(jnp.float32), jnp.float32(0.0))
        picked = as_wide[columns[:, slot_index].astype(jnp.int32)]
        summed = summed + jnp.einsum("rij,rjc->ric", weights, picked)
    return summed


def reference(start_block, onsite, hopping, columns, counts):
    center, listed = filter_coefficients(DEG)
    current = start_block.reshape(NBLK, BLK, M)
    previous = jnp.zeros((NBLK, BLK, M), jnp.bfloat16)
    for scale_now, carry_back in listed:
        applied = apply_operator(current, onsite, hopping, columns, counts)
        following = scale_now * (applied - center * current.astype(jnp.float32)) - carry_back * previous.astype(jnp.float32)
        following = lax.optimization_barrier(following.astype(jnp.bfloat16))
        previous, current = current, following
    filtered = current.reshape(NROWS, M)
    applied = apply_operator(current, onsite, hopping, columns, counts).astype(jnp.bfloat16).reshape(NROWS, M)
    gram = jnp.dot(filtered.T, filtered, preferred_element_type=jnp.float32) / NROWS
    projected = jnp.dot(filtered.T, applied, preferred_element_type=jnp.float32) / NROWS
    return filtered, gram, projected
```

```python
import functools

import jax
import jax.numpy as jnp
from jax import lax
from jax.experimental import pallas as pl
from jax.experimental.pallas import tpu as pltpu
from jax.sharding import PartitionSpec as P

DEG = 12
GROUP = 4
MESH = pl.DeviceIdType.MESH

filter_low = -0.5
filter_top = 4.0
filter_bottom = -1.6


def filter_coefficients(degree):
    center = 0.5 * (filter_top + filter_low)
    half_width = 0.5 * (filter_top - filter_low)
    sigma_first = half_width / (filter_bottom - center)
    listed = [(sigma_first / half_width, 0.0)]
    sigma_now = sigma_first
    for degree_step in range(1, degree):
        sigma_next = 1.0 / (2.0 / sigma_first - sigma_now)
        listed.append((2.0 * sigma_next / half_width, sigma_now * sigma_next))
        sigma_now = sigma_next
    return center, listed


def at_rows(start, size):
    return pl.ds(pl.multiple_of(start, size), size)


def kernel(
    dims,
    coef,
    start,
    hown,
    filtered,
    gram,
    projected,
    hbuf,
    y,
    fall,
    xt,
    part,
    inbox,
    local_sem,
    h_send,
    h_recv,
    hf_send,
    hf_recv,
    v_send,
    v_recv,
    halo_send,
    halo_recv,
    f_send,
    f_recv,
    ff_send,
    ff_recv,
    p_send,
    p_recv,
):
    count, blk, own_blocks = dims["count"], dims["blk"], dims["own_blocks"]
    group = GROUP
    slabs = count // group
    rows_dev = own_blocks * blk
    rows_slab = group * rows_dev
    wide = start.shape[1] // group
    pairs_dev = own_blocks // 2
    pairs = pairs_dev * group
    two = 2 * blk
    six = 6 * blk
    piece = gram.shape[0]
    me = lax.axis_index("atoms")
    core = lax.axis_index("vecs")
    other = 1 - core
    p = lax.rem(me, group)
    slab = lax.div(me, group)
    base = slab * group
    right = lax.rem(slab + 1, slabs) * group + p
    left = lax.rem(slab + slabs - 1, slabs) * group + p

    barrier = pltpu.get_barrier_semaphore()

    def greet(step, carry):
        peer = lax.rem(me + step, count)
        pl.semaphore_signal(
            barrier, inc=1, device_id={"atoms": peer, "vecs": core}, device_id_type=MESH
        )
        return carry

    lax.fori_loop(1, count, greet, 0)
    pl.semaphore_signal(barrier, inc=1, device_id={"atoms": me, "vecs": other}, device_id_type=MESH)

    own_h = pltpu.make_async_copy(
        hown, hbuf.at[pl.ds(p * pairs_dev, pairs_dev)], local_sem.at[0]
    )
    own_h.start()
    own_v = pltpu.make_async_copy(
        start.at[:, at_rows(p * wide, wide)],
        y.at[0, at_rows(two + p * rows_dev, two)]
        if rows_dev == two
        else y.at[0, pl.ds(pl.multiple_of(two + p * rows_dev, two), rows_dev)],
        local_sem.at[1],
    )
    own_v.start()
    y[1, two : two + rows_slab, :] = jnp.zeros((rows_slab, wide), jnp.bfloat16)

    pl.semaphore_wait(barrier, count)

    def peer_id(index, which):
        return {"atoms": index, "vecs": which}

    half = pairs_dev // 2

    def h_copy(source, target, step):
        return pltpu.make_async_remote_copy(
            src_ref=hown.at[pl.ds(core * half, half)],
            dst_ref=hbuf.at[pl.ds(source * pairs_dev + core * half, half)],
            send_sem=h_send.at[step],
            recv_sem=h_recv.at[step],
            device_id=peer_id(base + target, core),
            device_id_type=MESH,
        )

    def h_forward(source, step, which):
        where = pl.ds(source * pairs_dev + which * half, half)
        return pltpu.make_async_remote_copy(
            src_ref=hbuf.at[where],
            dst_ref=hbuf.at[where],
            send_sem=hf_send.at[step],
            recv_sem=hf_recv.at[step],
            device_id=peer_id(me, other),
            device_id_type=MESH,
        )

    def v_copy(source, target, step):
        return pltpu.make_async_remote_copy(
            src_ref=start.at[:, at_rows(target * wide, wide)],
            dst_ref=y.at[0, pl.ds(pl.multiple_of(two + source * rows_dev, two), rows_dev)],
            send_sem=v_send.at[step],
            recv_sem=v_recv.at[step],
            device_id=peer_id(base + target, core),
            device_id_type=MESH,
        )

    to = [lax.rem(p + step, group) for step in range(group)]
    source_of = [lax.rem(p + group - step, group) for step in range(group)]
    steps = (3, 1, 2)
    for step in steps:
        h_copy(p, to[step], step).start()
    for step in steps:
        v_copy(p, to[step], step).start()
    own_v.wait()
    own_h.wait()
    for step in steps:
        h_copy(source_of[step], p, step).wait_recv()
        h_forward(source_of[step], step, core).start()
    for step in steps:
        v_copy(source_of[step], p, step).wait_recv()

    def halo(slot, side):
        low = slice(two, 2 * two)
        high = slice(rows_slab, rows_slab + two)
        src = (high, low)[side]
        dst = (slice(0, two), slice(rows_slab + two, rows_slab + 2 * two))[side]
        return pltpu.make_async_remote_copy(
            src_ref=y.at[slot, src],
            dst_ref=y.at[slot, dst],
            send_sem=halo_send.at[slot, side],
            recv_sem=halo_recv.at[slot, side],
            device_id=peer_id((right, left)[side], core),
            device_id_type=MESH,
        )

    for side in (0, 1):
        halo(0, side).start()
    for step in steps:
        h_forward(source_of[step], step, other).wait_recv()

    def one_pair(src, dst, index, scale, shift, carry):
        window = y[src, pl.ds(pl.multiple_of(index * two, two), six), :]
        total = jnp.dot(hbuf[index], window, preferred_element_type=jnp.float32)
        mine = pl.ds(pl.multiple_of(index * two + two, two), two)
        now = y[src, mine, :].astype(jnp.float32)
        before = y[dst, mine, :].astype(jnp.float32)
        y[dst, mine, :] = (scale * total - shift * now - carry * before).astype(jnp.bfloat16)

    def one_step(step, last):
        dst = lax.rem(step, 2)
        src = 1 - dst
        scale, shift, carry = coef[3 * step], coef[3 * step + 1], coef[3 * step + 2]
        for side in (0, 1):
            halo(src, side).wait_recv()
        one_pair(src, dst, 0, scale, shift, carry)
        one_pair(src, dst, pairs - 1, scale, shift, carry)
        if not last:
            for side in (0, 1):
                halo(dst, side).start()
        for index in range(1, pairs - 1):
            one_pair(src, dst, index, scale, shift, carry)
        for side in (0, 1):
            halo(src, side).wait_send()

    def looped(step, state):
        one_step(step, False)
        return state

    lax.fori_loop(1, DEG + 1, looped, 0)
    final_slot = DEG % 2
    own = slice(two, two + rows_slab)

    def f_copy(source, target, step):
        return pltpu.make_async_remote_copy(
            src_ref=y.at[final_slot, own],
            dst_ref=fall.at[source, core],
            send_sem=f_send.at[step],
            recv_sem=f_recv.at[step],
            device_id=peer_id(base + target, core),
            device_id_type=MESH,
        )

    def f_forward(source, step, which):
        return pltpu.make_async_remote_copy(
            src_ref=y.at[final_slot, own] if step == 0 else fall.at[source, which],
            dst_ref=fall.at[source, which],
            send_sem=ff_send.at[step],
            recv_sem=ff_recv.at[step],
            device_id=peer_id(me, other),
            device_id_type=MESH,
        )

    for step in steps:
        f_copy(p, to[step], step).start()
    f_forward(p, 0, core).start()
    own_f = pltpu.make_async_copy(y.at[final_slot, own], fall.at[p, core], local_sem.at[2])
    own_f.start()
    one_step(DEG + 1, True)
    xt[0:wide, :] = y[final_slot, own, :].T
    xt[wide : 2 * wide, :] = y[1 - final_slot, own, :].T
    own_f.wait()

    owners = wide // piece

    def p_copy(owner, slot_from):
        return pltpu.make_async_remote_copy(
            src_ref=part.at[owner],
            dst_ref=inbox.at[slot_from],
            send_sem=p_send.at[owner],
            recv_sem=p_recv.at[slot_from],
            device_id=peer_id(owner, core),
            device_id_type=MESH,
        )

    def p_local():
        return pltpu.make_async_copy(part.at[me], inbox.at[me], p_recv.at[me])

    def strip(source, which):
        block = jnp.dot(xt[...], fall[source, which], preferred_element_type=jnp.float32)
        turned = block.T.reshape(owners, piece, 2 * wide).astype(jnp.bfloat16)
        first = (which * group + source) * owners
        part[pl.ds(first, owners)] = turned

        def send(index, state):
            owner = first + index

            @pl.when(owner != me)
            def _():
                p_copy(owner, me).start()

            @pl.when(owner == me)
            def _():
                p_local().start()

            return state

        lax.fori_loop(0, owners, send, 0)

    strip(p, core)
    f_forward(p, 0, other).wait_recv()
    strip(p, other)
    for step in steps:
        f_copy(source_of[step], p, step).wait_recv()
        f_forward(source_of[step], step, core).start()
        strip(source_of[step], core)
        f_forward(source_of[step], step, other).wait_recv()
        strip(source_of[step], other)
    for source in range(group):
        filtered[:, source * wide : (source + 1) * wide] = fall[
            source, core, pl.ds(pl.multiple_of(p * rows_dev, two), rows_dev), :
        ]

    def arrive(index, state):
        @pl.when(index != me)
        def _():
            p_copy(me, index).wait_recv()

        @pl.when(index == me)
        def _():
            p_local().wait()

        return state

    lax.fori_loop(0, count, arrive, 0)
    unit = 1.0 / (slabs * rows_slab)
    for source in range(group):

        def add(index, total):
            return total + inbox[index * group + source].astype(jnp.float32)

        summed = lax.fori_loop(0, slabs, add, jnp.zeros((piece, 2 * wide), jnp.float32)) * unit
        gram[:, source * wide : (source + 1) * wide] = summed[:, :wide]
        projected[:, source * wide : (source + 1) * wide] = summed[:, wide:]

    for step in steps:
        h_copy(p, to[step], step).wait_send()
        h_forward(source_of[step], step, core).wait_send()
        v_copy(p, to[step], step).wait_send()
        f_copy(p, to[step], step).wait_send()
        f_forward(source_of[step], step, core).wait_send()
    f_forward(p, 0, core).wait_send()

    def left_out(index, state):
        @pl.when(index != me)
        def _():
            p_copy(index, me).wait_send()

        return state

    lax.fori_loop(0, count, left_out, 0)


def shards(start_block, onsite, hopping, columns, counts):
    own_blocks, blk = onsite.shape[0], onsite.shape[1]
    slots = columns.shape[1]
    reach = slots // 2
    span = 2 * reach + 1
    count = lax.axis_size("atoms")
    cores = lax.axis_size("vecs")
    total_blocks = own_blocks * count
    width = start_block.shape[1]
    wide = width // GROUP
    piece = width * cores // count
    slabs = count // GROUP
    rows_slab = GROUP * own_blocks * blk
    pairs_dev = own_blocks // 2

    center, listed = filter_coefficients(DEG)
    coef = [(0.0, 0.0, 0.0)]
    coef += [(scale, scale * center, carry) for scale, carry in listed]
    coef += [(1.0, 0.0, 0.0)]
    table = jnp.array(coef, jnp.float32).reshape(-1)

    first = lax.axis_index("atoms") * own_blocks
    row_ids = first + jnp.arange(own_blocks, dtype=jnp.int32)
    offset = jnp.mod(columns - row_ids[:, None] + reach, total_blocks)
    live = jnp.arange(slots, dtype=jnp.int32)[None, :] < counts[:, None]
    wide_onsite = onsite.astype(jnp.float32)
    direct = (0.5 * (wide_onsite + jnp.swapaxes(wide_onsite, 1, 2))).astype(jnp.bfloat16)
    zero = jnp.zeros((), jnp.bfloat16)
    zeros = jnp.zeros((blk, blk), jnp.bfloat16)
    pair_rows = []
    for row in range(own_blocks):
        line = []
        for shift in range(span):
            block = direct[row] if shift == reach else zeros
            for slot in range(slots):
                chosen = live[row, slot] & (offset[row, slot] == shift)
                block = jnp.where(chosen, hopping[row, slot], block)
            line.append(block)
        line = line + [zeros] if row % 2 == 0 else [zeros] + line
        pair_rows.append(jnp.concatenate(line, axis=1))
    hown = jnp.concatenate(pair_rows, axis=0).reshape(pairs_dev, 2 * blk, 6 * blk)

    dims = {"count": count, "blk": blk, "own_blocks": own_blocks}
    vmem = pl.BlockSpec(memory_space=pltpu.VMEM)
    dma = pltpu.SemaphoreType.DMA
    return pl.pallas_call(
        functools.partial(kernel, dims),
        out_shape=(
            jax.ShapeDtypeStruct(start_block.shape, jnp.bfloat16),
            jax.ShapeDtypeStruct((piece, width), jnp.float32),
            jax.ShapeDtypeStruct((piece, width), jnp.float32),
        ),
        in_specs=[pl.BlockSpec(memory_space=pltpu.SMEM), vmem, vmem],
        out_specs=(vmem, vmem, vmem),
        scratch_shapes=[
            pltpu.VMEM((pairs_dev * GROUP, 2 * blk, 6 * blk), jnp.bfloat16),
            pltpu.VMEM((2, rows_slab + 4 * blk, wide), jnp.bfloat16),
            pltpu.VMEM((GROUP, cores, rows_slab, wide), jnp.bfloat16),
            pltpu.VMEM((2 * wide, rows_slab), jnp.bfloat16),
            pltpu.VMEM((count, piece, 2 * wide), jnp.bfloat16),
            pltpu.VMEM((count, piece, 2 * wide), jnp.bfloat16),
            dma((3,)),
            dma((GROUP,)),
            dma((GROUP,)),
            dma((GROUP,)),
            dma((GROUP,)),
            dma((GROUP,)),
            dma((GROUP,)),
            dma((2, 2)),
            dma((2, 2)),
            dma((GROUP,)),
            dma((GROUP,)),
            dma((GROUP,)),
            dma((GROUP,)),
            dma((count,)),
            dma((count,)),
        ],
        compiler_params=pltpu.CompilerParams(
            collective_id=0, has_side_effects=True, vmem_limit_bytes=48 * 1024 * 1024
        ),
    )(table, start_block, hown)


def solution(mesh):
    in_specs = (
        P("atoms", "vecs"),
        P("atoms", None, None),
        P("atoms", None, None, None),
        P("atoms", None),
        P("atoms"),
    )
    out_specs = (P("atoms", "vecs"), P("atoms", "vecs"), P("atoms", "vecs"))
    return jax.shard_map(shards, mesh=mesh, in_specs=in_specs, out_specs=out_specs, check_vma=False)
```

```python
import functools

import jax
import jax.numpy as jnp
from jax import lax
from jax.experimental import pallas as pl
from jax.experimental.pallas import tpu as pltpu
from jax.sharding import PartitionSpec as P

DEG = 12
GROUP = 4
MESH = pl.DeviceIdType.MESH

filter_low = -0.5
filter_top = 4.0
filter_bottom = -1.6


def filter_coefficients(degree):
    center = 0.5 * (filter_top + filter_low)
    half_width = 0.5 * (filter_top - filter_low)
    sigma_first = half_width / (filter_bottom - center)
    listed = [(sigma_first / half_width, 0.0)]
    sigma_now = sigma_first
    for degree_step in range(1, degree):
        sigma_next = 1.0 / (2.0 / sigma_first - sigma_now)
        listed.append((2.0 * sigma_next / half_width, sigma_now * sigma_next))
        sigma_now = sigma_next
    return center, listed


def at_rows(start, size):
    return pl.ds(pl.multiple_of(start, size), size)


def kernel(
    dims,
    coef,
    columns,
    counts,
    start,
    onsite,
    hopping,
    filtered,
    gram,
    projected,
    hown,
    hbuf,
    y,
    fall,
    xt,
    part,
    inbox,
    local_sem,
    h_send,
    h_recv,
    hf_send,
    hf_recv,
    v_send,
    v_recv,
    halo_send,
    halo_recv,
    f_send,
    f_recv,
    ff_send,
    ff_recv,
    p_send,
    p_recv,
):
    count, blk, own_blocks = dims["count"], dims["blk"], dims["own_blocks"]
    group = GROUP
    slabs = count // group
    total_blocks = own_blocks * count
    rows_dev = own_blocks * blk
    rows_slab = group * rows_dev
    wide = start.shape[1] // group
    pairs_dev = own_blocks // 2
    pairs = pairs_dev * group
    two = 2 * blk
    six = 6 * blk
    piece = gram.shape[0]
    me = lax.axis_index("atoms")
    core = lax.axis_index("vecs")
    other = 1 - core
    p = lax.rem(me, group)
    slab = lax.div(me, group)
    base = slab * group
    right = lax.rem(slab + 1, slabs) * group + p
    left = lax.rem(slab + slabs - 1, slabs) * group + p

    barrier = pltpu.get_barrier_semaphore()

    def greet(step, carry):
        peer = lax.rem(me + step, count)
        pl.semaphore_signal(
            barrier, inc=1, device_id={"atoms": peer, "vecs": core}, device_id_type=MESH
        )
        return carry

    lax.fori_loop(1, count, greet, 0)
    pl.semaphore_signal(barrier, inc=1, device_id={"atoms": me, "vecs": other}, device_id_type=MESH)

    own_v = pltpu.make_async_copy(
        start.at[:, at_rows(p * wide, wide)],
        y.at[0, at_rows(two + p * rows_dev, two)]
        if rows_dev == two
        else y.at[0, pl.ds(pl.multiple_of(two + p * rows_dev, two), rows_dev)],
        local_sem.at[0],
    )
    own_v.start()
    y[1, two : two + rows_slab, :] = jnp.zeros((rows_slab, wide), jnp.bfloat16)

    slots, reach = hopping.shape[1], dims["reach"]
    zeros = jnp.zeros((blk, blk), jnp.bfloat16)
    for row in range(own_blocks):
        pair, half_row = row // 2, row % 2
        lines = slice(half_row * blk, (half_row + 1) * blk)
        offsets = []
        for slot in range(slots):
            ahead = columns[row, slot] - (me * own_blocks + row) + reach + total_blocks
            offset = lax.rem(ahead, total_blocks)
            offsets.append(jnp.where(slot < counts[row], offset, -1))
        for shift in range(2 * reach + 1):
            if shift == reach:
                wide_block = onsite[row].astype(jnp.float32)
                block = (0.5 * (wide_block + wide_block.T)).astype(jnp.bfloat16)
            else:
                block = zeros
                for slot in range(slots):
                    block = jnp.where(offsets[slot] == shift, hopping[row, slot], block)
            place = half_row + shift
            hown[pair, lines, place * blk : (place + 1) * blk] = block
        empty = (1 - half_row) * 5
        hown[pair, lines, empty * blk : (empty + 1) * blk] = zeros

    pl.semaphore_wait(barrier, count)

    def peer_id(index, which):
        return {"atoms": index, "vecs": which}

    half = pairs_dev // 2

    def h_copy(source, target, step):
        return pltpu.make_async_remote_copy(
            src_ref=hown.at[pl.ds(core * half, half)],
            dst_ref=hbuf.at[pl.ds(source * pairs_dev + core * half, half)],
            send_sem=h_send.at[step],
            recv_sem=h_recv.at[step],
            device_id=peer_id(base + target, core),
            device_id_type=MESH,
        )

    def h_forward(source, step, which):
        where = pl.ds(source * pairs_dev + which * half, half)
        return pltpu.make_async_remote_copy(
            src_ref=hbuf.at[where],
            dst_ref=hbuf.at[where],
            send_sem=hf_send.at[step],
            recv_sem=hf_recv.at[step],
            device_id=peer_id(me, other),
            device_id_type=MESH,
        )

    def v_copy(source, target, step):
        return pltpu.make_async_remote_copy(
            src_ref=start.at[:, at_rows(target * wide, wide)],
            dst_ref=y.at[0, pl.ds(pl.multiple_of(two + source * rows_dev, two), rows_dev)],
            send_sem=v_send.at[step],
            recv_sem=v_recv.at[step],
            device_id=peer_id(base + target, core),
            device_id_type=MESH,
        )

    to = [lax.rem(p + step, group) for step in range(group)]
    source_of = [lax.rem(p + group - step, group) for step in range(group)]
    steps = (3, 1, 2)
    for step in steps:
        h_copy(p, to[step], step).start()
    for step in steps:
        v_copy(p, to[step], step).start()
    hbuf[pl.ds(p * pairs_dev, pairs_dev)] = hown[...]
    own_v.wait()
    for step in steps:
        h_copy(source_of[step], p, step).wait_recv()
        h_forward(source_of[step], step, core).start()
    for step in steps:
        v_copy(source_of[step], p, step).wait_recv()

    def halo(slot, side):
        low = slice(two, 2 * two)
        high = slice(rows_slab, rows_slab + two)
        src = (high, low)[side]
        dst = (slice(0, two), slice(rows_slab + two, rows_slab + 2 * two))[side]
        return pltpu.make_async_remote_copy(
            src_ref=y.at[slot, src],
            dst_ref=y.at[slot, dst],
            send_sem=halo_send.at[slot, side],
            recv_sem=halo_recv.at[slot, side],
            device_id=peer_id((right, left)[side], core),
            device_id_type=MESH,
        )

    for side in (0, 1):
        halo(0, side).start()
    for step in steps:
        h_forward(source_of[step], step, other).wait_recv()

    def one_pair(src, dst, index, scale, shift, carry):
        window = y[src, pl.ds(pl.multiple_of(index * two, two), six), :]
        total = jnp.dot(hbuf[index], window, preferred_element_type=jnp.float32)
        mine = pl.ds(pl.multiple_of(index * two + two, two), two)
        now = y[src, mine, :].astype(jnp.float32)
        before = y[dst, mine, :].astype(jnp.float32)
        y[dst, mine, :] = (scale * total - shift * now - carry * before).astype(jnp.bfloat16)

    def one_step(step, last):
        dst = lax.rem(step, 2)
        src = 1 - dst
        scale, shift, carry = coef[3 * step], coef[3 * step + 1], coef[3 * step + 2]
        for side in (0, 1):
            halo(src, side).wait_recv()
        one_pair(src, dst, 0, scale, shift, carry)
        one_pair(src, dst, pairs - 1, scale, shift, carry)
        if not last:
            for side in (0, 1):
                halo(dst, side).start()
        for index in range(1, pairs - 1):
            one_pair(src, dst, index, scale, shift, carry)
        for side in (0, 1):
            halo(src, side).wait_send()

    def looped(step, state):
        one_step(step, False)
        return state

    lax.fori_loop(1, DEG + 1, looped, 0)
    final_slot = DEG % 2
    own = slice(two, two + rows_slab)

    def f_copy(source, target, step):
        return pltpu.make_async_remote_copy(
            src_ref=y.at[final_slot, own],
            dst_ref=fall.at[source, core],
            send_sem=f_send.at[step],
            recv_sem=f_recv.at[step],
            device_id=peer_id(base + target, core),
            device_id_type=MESH,
        )

    def f_forward(source, step, which):
        return pltpu.make_async_remote_copy(
            src_ref=y.at[final_slot, own] if step == 0 else fall.at[source, which],
            dst_ref=fall.at[source, which],
            send_sem=ff_send.at[step],
            recv_sem=ff_recv.at[step],
            device_id=peer_id(me, other),
            device_id_type=MESH,
        )

    for step in steps:
        f_copy(p, to[step], step).start()
    f_forward(p, 0, core).start()
    own_f = pltpu.make_async_copy(y.at[final_slot, own], fall.at[p, core], local_sem.at[1])
    own_f.start()
    one_step(DEG + 1, True)
    xt[0:wide, :] = y[final_slot, own, :].T
    xt[wide : 2 * wide, :] = y[1 - final_slot, own, :].T
    own_f.wait()

    owners = wide // piece

    def p_copy(owner, slot_from):
        return pltpu.make_async_remote_copy(
            src_ref=part.at[owner],
            dst_ref=inbox.at[slot_from],
            send_sem=p_send.at[owner],
            recv_sem=p_recv.at[slot_from],
            device_id=peer_id(owner, core),
            device_id_type=MESH,
        )

    def p_local():
        return pltpu.make_async_copy(part.at[me], inbox.at[me], p_recv.at[me])

    def strip(source, which):
        block = jnp.dot(xt[...], fall[source, which], preferred_element_type=jnp.float32)
        turned = block.T.reshape(owners, piece, 2 * wide).astype(jnp.bfloat16)
        first = (which * group + source) * owners
        part[pl.ds(first, owners)] = turned

        def send(index, state):
            owner = first + index

            @pl.when(owner != me)
            def _():
                p_copy(owner, me).start()

            @pl.when(owner == me)
            def _():
                p_local().start()

            return state

        lax.fori_loop(0, owners, send, 0)

    strip(p, core)
    f_forward(p, 0, other).wait_recv()
    strip(p, other)
    for step in steps:
        f_copy(source_of[step], p, step).wait_recv()
        f_forward(source_of[step], step, core).start()
        strip(source_of[step], core)
        f_forward(source_of[step], step, other).wait_recv()
        strip(source_of[step], other)
    for source in range(group):
        filtered[:, source * wide : (source + 1) * wide] = fall[
            source, core, pl.ds(pl.multiple_of(p * rows_dev, two), rows_dev), :
        ]

    def arrive(index, state):
        @pl.when(index != me)
        def _():
            p_copy(me, index).wait_recv()

        @pl.when(index == me)
        def _():
            p_local().wait()

        return state

    lax.fori_loop(0, count, arrive, 0)
    unit = 1.0 / (slabs * rows_slab)
    for source in range(group):

        def add(index, total):
            return total + inbox[index * group + source].astype(jnp.float32)

        summed = lax.fori_loop(0, slabs, add, jnp.zeros((piece, 2 * wide), jnp.float32)) * unit
        gram[:, source * wide : (source + 1) * wide] = summed[:, :wide]
        projected[:, source * wide : (source + 1) * wide] = summed[:, wide:]

    for step in steps:
        h_copy(p, to[step], step).wait_send()
        h_forward(source_of[step], step, core).wait_send()
        v_copy(p, to[step], step).wait_send()
        f_copy(p, to[step], step).wait_send()
        f_forward(source_of[step], step, core).wait_send()
    f_forward(p, 0, core).wait_send()

    def left_out(index, state):
        @pl.when(index != me)
        def _():
            p_copy(index, me).wait_send()

        return state

    lax.fori_loop(0, count, left_out, 0)


def shards(start_block, onsite, hopping, columns, counts):
    own_blocks, blk = onsite.shape[0], onsite.shape[1]
    count = lax.axis_size("atoms")
    cores = lax.axis_size("vecs")
    width = start_block.shape[1]
    wide = width // GROUP
    piece = width * cores // count
    slabs = count // GROUP
    rows_slab = GROUP * own_blocks * blk
    pairs_dev = own_blocks // 2

    center, listed = filter_coefficients(DEG)
    coef = [(0.0, 0.0, 0.0)]
    coef += [(scale, scale * center, carry) for scale, carry in listed]
    coef += [(1.0, 0.0, 0.0)]
    table = jnp.array(coef, jnp.float32).reshape(-1)

    dims = {"count": count, "blk": blk, "own_blocks": own_blocks, "reach": columns.shape[1] // 2}
    vmem = pl.BlockSpec(memory_space=pltpu.VMEM)
    smem = pl.BlockSpec(memory_space=pltpu.SMEM)
    dma = pltpu.SemaphoreType.DMA
    return pl.pallas_call(
        functools.partial(kernel, dims),
        out_shape=(
            jax.ShapeDtypeStruct(start_block.shape, jnp.bfloat16),
            jax.ShapeDtypeStruct((piece, width), jnp.float32),
            jax.ShapeDtypeStruct((piece, width), jnp.float32),
        ),
        in_specs=[smem, smem, smem, vmem, vmem, vmem],
        out_specs=(vmem, vmem, vmem),
        scratch_shapes=[
            pltpu.VMEM((pairs_dev, 2 * blk, 6 * blk), jnp.bfloat16),
            pltpu.VMEM((pairs_dev * GROUP, 2 * blk, 6 * blk), jnp.bfloat16),
            pltpu.VMEM((2, rows_slab + 4 * blk, wide), jnp.bfloat16),
            pltpu.VMEM((GROUP, cores, rows_slab, wide), jnp.bfloat16),
            pltpu.VMEM((2 * wide, rows_slab), jnp.bfloat16),
            pltpu.VMEM((count, piece, 2 * wide), jnp.bfloat16),
            pltpu.VMEM((count, piece, 2 * wide), jnp.bfloat16),
            dma((2,)),
            dma((GROUP,)),
            dma((GROUP,)),
            dma((GROUP,)),
            dma((GROUP,)),
            dma((GROUP,)),
            dma((GROUP,)),
            dma((2, 2)),
            dma((2, 2)),
            dma((GROUP,)),
            dma((GROUP,)),
            dma((GROUP,)),
            dma((GROUP,)),
            dma((count,)),
            dma((count,)),
        ],
        compiler_params=pltpu.CompilerParams(
            collective_id=0, has_side_effects=True, vmem_limit_bytes=48 * 1024 * 1024
        ),
    )(table, columns, counts, start_block, onsite, hopping)


def solution(mesh):
    in_specs = (
        P("atoms", "vecs"),
        P("atoms", None, None),
        P("atoms", None, None, None),
        P("atoms", None),
        P("atoms"),
    )
    out_specs = (P("atoms", "vecs"), P("atoms", "vecs"), P("atoms", "vecs"))
    return jax.shard_map(shards, mesh=mesh, in_specs=in_specs, out_specs=out_specs, check_vma=False)
```

```python
import functools

import jax
import jax.numpy as jnp
from jax import lax
from jax.experimental import pallas as pl
from jax.experimental.pallas import tpu as pltpu
from jax.sharding import PartitionSpec as P

DEG = 12
GROUP = 4
MESH = pl.DeviceIdType.MESH

filter_low = -0.5
filter_top = 4.0
filter_bottom = -1.6


def filter_coefficients(degree):
    center = 0.5 * (filter_top + filter_low)
    half_width = 0.5 * (filter_top - filter_low)
    sigma_first = half_width / (filter_bottom - center)
    listed = [(sigma_first / half_width, 0.0)]
    sigma_now = sigma_first
    for degree_step in range(1, degree):
        sigma_next = 1.0 / (2.0 / sigma_first - sigma_now)
        listed.append((2.0 * sigma_next / half_width, sigma_now * sigma_next))
        sigma_now = sigma_next
    return center, listed


def at_rows(start, size):
    return pl.ds(pl.multiple_of(start, size), size)


def kernel(
    dims,
    coef,
    columns,
    counts,
    start,
    onsite,
    hopping,
    filtered,
    gram,
    projected,
    hbuf,
    y,
    fall,
    xt,
    part,
    inbox,
    local_sem,
    h_send,
    h_recv,
    hf_send,
    hf_recv,
    v_send,
    v_recv,
    halo_send,
    halo_recv,
    f_send,
    f_recv,
    ff_send,
    ff_recv,
    p_send,
    p_recv,
):
    count, blk, own_blocks = dims["count"], dims["blk"], dims["own_blocks"]
    group = GROUP
    slabs = count // group
    total_blocks = own_blocks * count
    rows_dev = own_blocks * blk
    rows_slab = group * rows_dev
    wide = start.shape[1] // group
    pairs_dev = own_blocks // 2
    pairs = pairs_dev * group
    two = 2 * blk
    six = 6 * blk
    piece = gram.shape[0]
    me = lax.axis_index("atoms")
    core = lax.axis_index("vecs")
    other = 1 - core
    p = lax.rem(me, group)
    slab = lax.div(me, group)
    base = slab * group
    right = lax.rem(slab + 1, slabs) * group + p
    left = lax.rem(slab + slabs - 1, slabs) * group + p

    barrier = pltpu.get_barrier_semaphore()

    def greet(step, carry):
        peer = lax.rem(me + step, count)
        pl.semaphore_signal(
            barrier, inc=1, device_id={"atoms": peer, "vecs": core}, device_id_type=MESH
        )
        return carry

    lax.fori_loop(1, count, greet, 0)
    pl.semaphore_signal(barrier, inc=1, device_id={"atoms": me, "vecs": other}, device_id_type=MESH)

    own_v = pltpu.make_async_copy(
        start.at[:, at_rows(p * wide, wide)],
        y.at[0, at_rows(two + p * rows_dev, two)]
        if rows_dev == two
        else y.at[0, pl.ds(pl.multiple_of(two + p * rows_dev, two), rows_dev)],
        local_sem.at[0],
    )
    own_v.start()
    y[1, two : two + rows_slab, :] = jnp.zeros((rows_slab, wide), jnp.bfloat16)

    slots, reach = hopping.shape[1], dims["reach"]
    zeros = jnp.zeros((blk, blk), jnp.bfloat16)
    for row in range(own_blocks):
        pair, half_row = row // 2, row % 2
        lines = slice(half_row * blk, (half_row + 1) * blk)
        offsets = []
        for slot in range(slots):
            ahead = columns[row, slot] - (me * own_blocks + row) + reach + total_blocks
            offset = lax.rem(ahead, total_blocks)
            offsets.append(jnp.where(slot < counts[row], offset, -1))
        for shift in range(2 * reach + 1):
            if shift == reach:
                wide_block = onsite[row].astype(jnp.float32)
                block = (0.5 * (wide_block + wide_block.T)).astype(jnp.bfloat16)
            else:
                block = zeros
                for slot in range(slots):
                    block = jnp.where(offsets[slot] == shift, hopping[row, slot], block)
            place = half_row + shift
            hbuf[p * pairs_dev + pair, lines, place * blk : (place + 1) * blk] = block
    for pair in range(pairs):
        hbuf[pair, 0:blk, 5 * blk : six] = zeros
        hbuf[pair, blk:two, 0:blk] = zeros

    pl.semaphore_wait(barrier, count)

    def peer_id(index, which):
        return {"atoms": index, "vecs": which}

    side_of = (p, p + 1 - 2 * lax.rem(p, 2), lax.rem(p + 2, group), group - 1 - p)
    steps = (1, 2, 3)
    relays = ((1, 2), (2, 1))

    def h_place(pair, row):
        return (pair, slice(row * blk, (row + 1) * blk), slice(row * blk, (row + 5) * blk))

    def h_copy(source, via, step, row):
        place = h_place(source * pairs_dev + core, row)
        return pltpu.make_async_remote_copy(
            src_ref=hbuf.at[place],
            dst_ref=hbuf.at[place],
            send_sem=h_send.at[step, row],
            recv_sem=h_recv.at[step, row],
            device_id=peer_id(base + side_of[via], core),
            device_id_type=MESH,
        )

    def h_forward(step, which, row):
        place = h_place(side_of[step] * pairs_dev + which, row)
        return pltpu.make_async_remote_copy(
            src_ref=hbuf.at[place],
            dst_ref=hbuf.at[place],
            send_sem=hf_send.at[step, row],
            recv_sem=hf_recv.at[step, row],
            device_id=peer_id(me, other),
            device_id_type=MESH,
        )

    def v_copy(source, target, step):
        return pltpu.make_async_remote_copy(
            src_ref=start.at[:, at_rows(target * wide, wide)],
            dst_ref=y.at[0, pl.ds(pl.multiple_of(two + source * rows_dev, two), rows_dev)],
            send_sem=v_send.at[step],
            recv_sem=v_recv.at[step],
            device_id=peer_id(base + target, core),
            device_id_type=MESH,
        )

    for row in (0, 1):
        h_copy(p, 1 + row, 1 + row, row).start()
    for row in (0, 1):
        h_copy(p, 2 - row, 2 - row, row).start()
    for row, (step, via) in enumerate(relays):
        h_copy(side_of[step], step, step, row).wait_recv()
        h_copy(side_of[step], via, 3, row).start()
        h_forward(step, core, row).start()
    for step in steps:
        v_copy(p, side_of[step], step).start()
    own_v.wait()
    for row, (step, via) in enumerate(relays):
        h_copy(side_of[via], via, via, row).wait_recv()
        h_forward(via, core, row).start()
    for row in (0, 1):
        h_copy(side_of[3], 3, 3, row).wait_recv()
        h_forward(3, core, row).start()
    for step in steps:
        v_copy(side_of[step], p, step).wait_recv()

    def halo(slot, side):
        low = slice(two, 2 * two)
        high = slice(rows_slab, rows_slab + two)
        src = (high, low)[side]
        dst = (slice(0, two), slice(rows_slab + two, rows_slab + 2 * two))[side]
        return pltpu.make_async_remote_copy(
            src_ref=y.at[slot, src],
            dst_ref=y.at[slot, dst],
            send_sem=halo_send.at[slot, side],
            recv_sem=halo_recv.at[slot, side],
            device_id=peer_id((right, left)[side], core),
            device_id_type=MESH,
        )

    for side in (0, 1):
        halo(0, side).start()
    for step in steps:
        for row in (0, 1):
            h_forward(step, other, row).wait_recv()

    def one_pair(src, dst, index, scale, shift, carry):
        window = y[src, pl.ds(pl.multiple_of(index * two, two), six), :]
        total = jnp.dot(hbuf[index], window, preferred_element_type=jnp.float32)
        mine = pl.ds(pl.multiple_of(index * two + two, two), two)
        now = y[src, mine, :].astype(jnp.float32)
        before = y[dst, mine, :].astype(jnp.float32)
        y[dst, mine, :] = (scale * total - shift * now - carry * before).astype(jnp.bfloat16)

    def one_step(step, last):
        dst = lax.rem(step, 2)
        src = 1 - dst
        scale, shift, carry = coef[3 * step], coef[3 * step + 1], coef[3 * step + 2]
        for side, edge in ((0, 0), (1, pairs - 1)):
            halo(src, side).wait_recv()
            one_pair(src, dst, edge, scale, shift, carry)
            if not last:
                halo(dst, 1 - side).start()
        for index in range(1, pairs - 1):
            one_pair(src, dst, index, scale, shift, carry)
        for side in (0, 1):
            halo(src, side).wait_send()

    def looped(step, state):
        one_step(step, False)
        return state

    lax.fori_loop(1, DEG + 1, looped, 0)
    final_slot = DEG % 2
    own = slice(two, two + rows_slab)

    half = rows_slab // 2

    def f_copy(source, via, step, part_of):
        rows = slice(part_of * half, (part_of + 1) * half)
        place = fall.at[source, core, rows]
        own_rows = slice(two + part_of * half, two + (part_of + 1) * half)
        return pltpu.make_async_remote_copy(
            src_ref=place if step == 3 else y.at[final_slot, own_rows],
            dst_ref=place,
            send_sem=f_send.at[step, part_of],
            recv_sem=f_recv.at[step, part_of],
            device_id=peer_id(base + side_of[via], core),
            device_id_type=MESH,
        )

    def f_forward(step, which, part_of):
        rows = slice(part_of * half, (part_of + 1) * half)
        own_rows = slice(two + part_of * half, two + (part_of + 1) * half)
        place = fall.at[side_of[step], which, rows]
        return pltpu.make_async_remote_copy(
            src_ref=y.at[final_slot, own_rows] if step == 0 else place,
            dst_ref=place,
            send_sem=ff_send.at[step, part_of],
            recv_sem=ff_recv.at[step, part_of],
            device_id=peer_id(me, other),
            device_id_type=MESH,
        )

    for row in (0, 1):
        f_copy(p, 1 + row, 1 + row, row).start()
    for row in (0, 1):
        f_copy(p, 2 - row, 2 - row, row).start()
    for row in (0, 1):
        f_forward(0, core, row).start()
    own_f = pltpu.make_async_copy(y.at[final_slot, own], fall.at[p, core], local_sem.at[1])
    own_f.start()
    one_step(DEG + 1, True)
    xt[0:wide, :] = y[final_slot, own, :].T
    xt[wide : 2 * wide, :] = y[1 - final_slot, own, :].T
    own_f.wait()

    owners = wide // piece

    def p_copy(owner, slot_from):
        return pltpu.make_async_remote_copy(
            src_ref=part.at[owner],
            dst_ref=inbox.at[slot_from],
            send_sem=p_send.at[owner],
            recv_sem=p_recv.at[slot_from],
            device_id=peer_id(owner, core),
            device_id_type=MESH,
        )

    def p_local():
        return pltpu.make_async_copy(part.at[me], inbox.at[me], p_recv.at[me])

    def strip(source, which):
        block = jnp.dot(xt[...], fall[source, which], preferred_element_type=jnp.float32)
        turned = block.T.reshape(owners, piece, 2 * wide).astype(jnp.bfloat16)
        first = (which * group + source) * owners
        part[pl.ds(first, owners)] = turned

        def send(index, state):
            owner = first + index

            @pl.when(owner != me)
            def _():
                p_copy(owner, me).start()

            @pl.when(owner == me)
            def _():
                p_local().start()

            return state

        lax.fori_loop(0, owners, send, 0)

    strip(p, core)
    for row in (0, 1):
        f_forward(0, other, row).wait_recv()
    for row, (step, via) in enumerate(relays):
        f_copy(side_of[step], step, step, row).wait_recv()
        f_copy(side_of[step], via, 3, row).start()
        f_forward(step, core, row).start()
    strip(p, other)
    for row, (step, via) in enumerate(relays):
        f_copy(side_of[via], via, via, row).wait_recv()
        f_forward(via, core, row).start()
    strip(side_of[1], core)
    strip(side_of[2], core)
    for step in (1, 2):
        for row in (0, 1):
            f_forward(step, other, row).wait_recv()
        strip(side_of[step], other)
    for row in (0, 1):
        f_copy(side_of[3], 3, 3, row).wait_recv()
        f_forward(3, core, row).start()
    strip(side_of[3], core)
    for row in (0, 1):
        f_forward(3, other, row).wait_recv()
    strip(side_of[3], other)
    for source in range(group):
        filtered[:, source * wide : (source + 1) * wide] = fall[
            source, core, pl.ds(pl.multiple_of(p * rows_dev, two), rows_dev), :
        ]

    def arrive(index, state):
        @pl.when(index != me)
        def _():
            p_copy(me, index).wait_recv()

        @pl.when(index == me)
        def _():
            p_local().wait()

        return state

    lax.fori_loop(0, count, arrive, 0)
    unit = 1.0 / (slabs * rows_slab)
    for source in range(group):

        def add(index, total):
            return total + inbox[index * group + source].astype(jnp.float32)

        summed = lax.fori_loop(0, slabs, add, jnp.zeros((piece, 2 * wide), jnp.float32)) * unit
        gram[:, source * wide : (source + 1) * wide] = summed[:, :wide]
        projected[:, source * wide : (source + 1) * wide] = summed[:, wide:]

    for step in steps:
        v_copy(p, side_of[step], step).wait_send()
        for row in (0, 1):
            h_forward(step, core, row).wait_send()
            f_forward(step, core, row).wait_send()
    for row, (step, via) in enumerate(relays):
        for near in (1, 2):
            h_copy(p, near, near, row).wait_send()
            f_copy(p, near, near, row).wait_send()
        h_copy(side_of[step], via, 3, row).wait_send()
        f_copy(side_of[step], via, 3, row).wait_send()
        f_forward(0, core, row).wait_send()

    def left_out(index, state):
        @pl.when(index != me)
        def _():
            p_copy(index, me).wait_send()

        return state

    lax.fori_loop(0, count, left_out, 0)


def shards(start_block, onsite, hopping, columns, counts):
    own_blocks, blk = onsite.shape[0], onsite.shape[1]
    count = lax.axis_size("atoms")
    cores = lax.axis_size("vecs")
    width = start_block.shape[1]
    wide = width // GROUP
    piece = width * cores // count
    slabs = count // GROUP
    rows_slab = GROUP * own_blocks * blk
    pairs_dev = own_blocks // 2

    center, listed = filter_coefficients(DEG)
    coef = [(0.0, 0.0, 0.0)]
    coef += [(scale, scale * center, carry) for scale, carry in listed]
    coef += [(1.0, 0.0, 0.0)]
    table = jnp.array(coef, jnp.float32).reshape(-1)

    dims = {"count": count, "blk": blk, "own_blocks": own_blocks, "reach": columns.shape[1] // 2}
    vmem = pl.BlockSpec(memory_space=pltpu.VMEM)
    smem = pl.BlockSpec(memory_space=pltpu.SMEM)
    dma = pltpu.SemaphoreType.DMA
    return pl.pallas_call(
        functools.partial(kernel, dims),
        out_shape=(
            jax.ShapeDtypeStruct(start_block.shape, jnp.bfloat16),
            jax.ShapeDtypeStruct((piece, width), jnp.float32),
            jax.ShapeDtypeStruct((piece, width), jnp.float32),
        ),
        in_specs=[smem, smem, smem, vmem, vmem, vmem],
        out_specs=(vmem, vmem, vmem),
        scratch_shapes=[
            pltpu.VMEM((pairs_dev * GROUP, 2 * blk, 6 * blk), jnp.bfloat16),
            pltpu.VMEM((2, rows_slab + 4 * blk, wide), jnp.bfloat16),
            pltpu.VMEM((GROUP, cores, rows_slab, wide), jnp.bfloat16),
            pltpu.VMEM((2 * wide, rows_slab), jnp.bfloat16),
            pltpu.VMEM((count, piece, 2 * wide), jnp.bfloat16),
            pltpu.VMEM((count, piece, 2 * wide), jnp.bfloat16),
            dma((2,)),
            dma((GROUP, 2)),
            dma((GROUP, 2)),
            dma((GROUP, 2)),
            dma((GROUP, 2)),
            dma((GROUP,)),
            dma((GROUP,)),
            dma((2, 2)),
            dma((2, 2)),
            dma((GROUP, 2)),
            dma((GROUP, 2)),
            dma((GROUP, 2)),
            dma((GROUP, 2)),
            dma((count,)),
            dma((count,)),
        ],
        compiler_params=pltpu.CompilerParams(
            collective_id=0, has_side_effects=True, vmem_limit_bytes=48 * 1024 * 1024
        ),
    )(table, columns, counts, start_block, onsite, hopping)


def solution(mesh):
    in_specs = (
        P("atoms", "vecs"),
        P("atoms", None, None),
        P("atoms", None, None, None),
        P("atoms", None),
        P("atoms"),
    )
    out_specs = (P("atoms", "vecs"), P("atoms", "vecs"), P("atoms", "vecs"))
    return jax.shard_map(shards, mesh=mesh, in_specs=in_specs, out_specs=out_specs, check_vma=False)
```
